32 devices in a mesh: node: 4 (over y, x), space: 8 (over z, core).
Axes of the slice: x: 2, y: 2, z: 4, core: 2. Of those that a mesh axis runs over, the one named last changes fastest.
Arguments:
- initial: float32 [2, 512, 4096], P(None, 'space'), may hold values from 0 to 1
- sections: float32 [4, 2, 512, 4096], P('node', None, 'space'), may hold values from 0 to 1
- feed_rate: float32 [512, 4096], P('space'), may hold values from 0.02 to 0.12
- kill_rate: float32 [512, 4096], P('space'), may hold values from 0.04 to 0.12
Outputs:
- new_sections: float32 [4, 2, 512, 4096], P('node', None, 'space')
- residual_max: float32 [], replicated
The draws below stay inside these ranges and needn't reach their ends.
All inputs are finite; a program needn't handle non-finite values.
Results may differ from the reference program's by a relative error of at most 0.000094.
Values sent between devices are 32-bit elements; how exact they have to be, the bound alone decides.
No kernel may reach another device: no remote copies, remote signals or barrier semaphores. Data moves between devices by JAX's collectives and lax.ppermute only.
A program may use at most 64 MiB of HBM per device.

```python
import math
import jax
import jax.numpy as jnp
import numpy as np
from jax import lax

NY = 4096
SWEEPS = 6
M = 4
NX = 512


def steps_of(key, extent, cuts, low, high):
    def one(position, shards_of):
        draws = jax.random.uniform(jax.random.fold_in(jax.random.fold_in(key, 6), position), (shards_of,), jnp.float32, low / len(cuts), high / len(cuts))
        return jnp.repeat(jnp.exp(draws), extent[position] // shards_of).reshape((-1,) + (1,) * (len(extent) - position - 1))

    level = one(*cuts[0])
    for cut in cuts[1:]:
        level = level * one(*cut)
    return level


def setup_inputs(seed: int = 0) -> dict:
    arg_keys = jax.random.split(jax.random.key(seed), 5)
    return {
        "initial": jnp.clip(1.0 * jax.random.uniform(arg_keys[0], (2, NX, NY), jnp.float32) ** steps_of(arg_keys[0], (2, NX, NY), ((1, 8),), -0.2, 0.2), 0.0, 1.0),
        "sections": jnp.clip(1.0 * jax.random.uniform(arg_keys[1], (M, 2, NX, NY), jnp.float32) ** steps_of(arg_keys[1], (M, 2, NX, NY), ((0, 4), (2, 8)), -0.2, 0.2), 0.0, 1.0),
        "feed_rate": jnp.clip(jnp.exp(math.log(0.12) - 1.7917595 * jax.random.uniform(arg_keys[2], (NX, NY), jnp.float32) ** steps_of(arg_keys[2], (NX, NY), ((0, 8),), -0.2, 0.2)), 0.02, 0.12),
        "kill_rate": jnp.clip(jnp.exp(math.log(0.12) - 1.0986123 * jax.random.uniform(arg_keys[3], (NX, NY), jnp.float32) ** steps_of(arg_keys[3], (NX, NY), ((0, 8),), -0.2, 0.2)), 0.04, 0.12),
    }


step_size = 4.0
diff_u = 1.0
diff_v = 0.5


def radau_target(order, value):
    before = 1.0
    current = value
    previous = 1.0
    for degree in range(1, order):
        following = ((2 * degree + 1) * value * current - degree * before) / (degree + 1)
        before = current
        current = following
    if order == 1:
        previous = 1.0
    else:
        previous = before
    return current - previous


def radau_table(total):
    grid_count = 20000
    roots_found = []
    left_value = -1.0
    left_target = radau_target(total, left_value)
    for step_index in range(1, grid_count):
        right_value = -1.0 + 2.0 * step_index / grid_count
        right_target = radau_target(total, right_value)
        if left_target * right_target < 0.0:
            lower = left_value
            upper = right_value
            lower_target = left_target
            for bisect_index in range(80):
                halfway = 0.5 * (lower + upper)
                halfway_target = radau_target(total, halfway)
                if lower_target * halfway_target <= 0.0:
                    upper = halfway
                else:
                    lower = halfway
                    lower_target = halfway_target
            roots_found.append(0.5 * (lower + upper))
        left_value = right_value
        left_target = right_target
    roots_found.append(1.0)
    points = [(value + 1.0) / 2.0 for value in roots_found]
    quad_rows = []
    for node_index in range(total):
        row_values = []
        for basis_index in range(total):
            coefs = [1.0]
            for other_index in range(total):
                if other_index != basis_index:
                    scale = 1.0 / (points[basis_index] - points[other_index])
                    shifted = [0.0] + coefs
                    widened = coefs + [0.0]
                    coefs = [(shifted[k] - points[other_index] * widened[k]) * scale for k in range(len(shifted))]
            integral = 0.0
            for power_index in range(len(coefs)):
                integral += coefs[power_index] * points[node_index] ** (power_index + 1) / (power_index + 1)
            row_values.append(integral)
        quad_rows.append(row_values)
    return np.array(points), np.array(quad_rows)


def neighbours(field):
    return (jnp.roll(field, -1, 2) + jnp.roll(field, 1, 2)) + (jnp.roll(field, -1, 3) + jnp.roll(field, 1, 3))


def reference(initial, sections, feed_rate, kill_rate):
    points, quad_matrix = radau_table(M)
    points = jnp.asarray(points, jnp.float32)
    quad_matrix = jnp.asarray(quad_matrix, jnp.float32)
    diffusivity = jnp.array([diff_u, diff_v], jnp.float32).reshape(1, 2, 1, 1)
    laplace = neighbours(sections) - 4.0 * sections
    implicit = diffusivity * laplace
    species_u = sections[:, 0]
    species_v = sections[:, 1]
    product = species_u * species_v * species_v
    reaction = jnp.stack((-product + feed_rate * (1.0 - species_u), product - (feed_rate + kill_rate) * species_v), axis=1)
    slopes = implicit + reaction
    summed = jnp.einsum("mj,jsxy->msxy", quad_matrix, slopes, precision=lax.Precision.HIGHEST)
    quadrature = initial[None] + step_size * summed
    residual_max = jnp.max(jnp.abs(quadrature - sections))
    node_step = (step_size * points).reshape(M, 1, 1, 1)
    right_side = quadrature - node_step * implicit
    coupling = node_step * diffusivity
    divisor = 4.0 * coupling + 1.0
    iterate = sections
    for sweep_index in range(SWEEPS):
        iterate = (right_side + coupling * neighbours(iterate)) / divisor
    return iterate, residual_max
```

```python
from functools import partial

import jax
import jax.numpy as jnp
import numpy as np
from jax import lax
from jax.experimental import pallas as pl
from jax.experimental.pallas import tpu as pltpu
from jax.sharding import PartitionSpec as P

SWEEPS = 6
TILE = 8

step_size = 4.0
diffusion = (1.0, 0.5)


def radau_target(order, value):
    before = 1.0
    current = value
    previous = 1.0
    for degree in range(1, order):
        following = ((2 * degree + 1) * value * current - degree * before) / (degree + 1)
        before = current
        current = following
    previous = before
    return current - previous


def radau_table(total):
    grid_count = 20000
    roots_found = []
    left_value = -1.0
    left_target = radau_target(total, left_value)
    for step_index in range(1, grid_count):
        right_value = -1.0 + 2.0 * step_index / grid_count
        right_target = radau_target(total, right_value)
        if left_target * right_target < 0.0:
            lower = left_value
            upper = right_value
            lower_target = left_target
            for bisect_index in range(80):
                halfway = 0.5 * (lower + upper)
                halfway_target = radau_target(total, halfway)
                if lower_target * halfway_target <= 0.0:
                    upper = halfway
                else:
                    lower = halfway
                    lower_target = halfway_target
            roots_found.append(0.5 * (lower + upper))
        left_value = right_value
        left_target = right_target
    roots_found.append(1.0)
    points = [(value + 1.0) / 2.0 for value in roots_found]
    quad_rows = []
    for node_index in range(total):
        row_values = []
        for basis_index in range(total):
            coefs = [1.0]
            for other_index in range(total):
                if other_index != basis_index:
                    scale = 1.0 / (points[basis_index] - points[other_index])
                    shifted = [0.0] + coefs
                    widened = coefs + [0.0]
                    coefs = [
                        (shifted[k] - points[other_index] * widened[k]) * scale
                        for k in range(len(shifted))
                    ]
            integral = 0.0
            for power_index in range(len(coefs)):
                integral += (
                    coefs[power_index] * points[node_index] ** (power_index + 1) / (power_index + 1)
                )
            row_values.append(integral)
        quad_rows.append(row_values)
    return (np.array(points), np.array(quad_rows))


def neighbour_sum(above, tile, below):
    rows, columns = tile.shape
    row = lax.broadcasted_iota(jnp.int32, tile.shape, 0)
    up = jnp.where(row == 0, above, pltpu.roll(tile, 1, 0))
    down = jnp.where(row == rows - 1, below, pltpu.roll(tile, rows - 1, 0))
    return (up + down) + (pltpu.roll(tile, 1, 1) + pltpu.roll(tile, columns - 1, 1))


def tile_slopes(u_rows, v_rows, feed, kill):
    above_u, u, below_u = u_rows
    above_v, v, below_v = v_rows
    product = u * v * v
    slope_u = diffusion[0] * (neighbour_sum(above_u, u, below_u) - 4.0 * u)
    slope_v = diffusion[1] * (neighbour_sum(above_v, v, below_v) - 4.0 * v)
    slope_u = slope_u + (feed * (1.0 - u) - product)
    slope_v = slope_v + (product - (feed + kill) * v)
    return slope_u, slope_v


def rows_of(ref, species, start, before, after):
    length = ref.shape[1]
    above = before[species] if start == 0 else ref[species, start - 1 : start]
    stop = start + TILE
    below = after[species] if stop == length else ref[species, stop : stop + 1]
    return above, ref[species, start:stop], below


def slopes_kernel(groups, halo, *refs):
    if halo:
        before, after, *refs = refs
    else:
        before = after = None
    sections, feed, kill, *outs = refs
    for group, starts in enumerate(groups):
        for k, start in enumerate(starts):
            slope_u, slope_v = tile_slopes(
                rows_of(sections, 0, start, before, after),
                rows_of(sections, 1, start, before, after),
                feed[start : start + TILE],
                kill[start : start + TILE],
            )
            outs[2 * group][k * TILE : (k + 1) * TILE] = slope_u
            outs[2 * group + 1][k * TILE : (k + 1) * TILE] = slope_v


def slopes_of(groups, halos, sections, feed_rate, kill_rate):
    columns = sections.shape[-1]
    shapes = []
    for starts in groups:
        shapes += [jax.ShapeDtypeStruct((len(starts) * TILE, columns), jnp.float32)] * 2
    return pl.pallas_call(
        partial(slopes_kernel, groups, bool(halos)),
        out_shape=shapes,
        compiler_params=pltpu.CompilerParams(vmem_limit_bytes=24 * 2**20),
    )(*halos, sections, feed_rate, kill_rate)


def sweep_kernel(places, factors, before, after, sections, *refs):
    pieces = refs[: len(places)]
    out, first, even, odd = refs[len(places) :]
    species = pl.program_id(0)
    inverse = factors[0, species]
    gain = factors[1, species]
    total = first.shape[0]
    first[0:TILE] = before[0] * inverse
    first[total - TILE : total] = after[0] * inverse
    for piece, starts in zip(pieces, places):
        for k, start in enumerate(starts):
            first[start + TILE : start + 2 * TILE] = piece[0, k * TILE : (k + 1) * TILE] * inverse

    def updated(source, start):
        above = source[pl.ds(jnp.maximum(start - 1, 0), 1)]
        below = source[pl.ds(jnp.minimum(start + TILE, total - 1), 1)]
        here = pl.ds(start, TILE)
        return first[here] + gain * neighbour_sum(above, source[here], below)

    source = first
    for sweep in range(SWEEPS - 2):
        target = (even, odd)[sweep % 2]

        def one_tile(t, _, source=source, target=target):
            start = pl.multiple_of(t * TILE, TILE)
            target[pl.ds(start, TILE)] = updated(source, start)
            return 0

        lax.fori_loop(0, total // TILE, one_tile, 0)
        source = target

    def last_tile(t, _):
        start = pl.multiple_of(t * TILE, TILE)
        here = pl.ds(start, TILE)
        out[0, here] = sections[0, here] + updated(source, pl.multiple_of(start + TILE, TILE))
        return 0

    lax.fori_loop(0, total // TILE - 2, last_tile, 0)


def swept(places, factors, before, after, sections, pieces):
    _, rows, columns = sections.shape
    total = rows + 2 * TILE
    per_species = lambda array: pl.BlockSpec((1,) + array.shape[1:], lambda s: (s, 0, 0))
    blocked = [before, after, sections, *pieces]
    return pl.pallas_call(
        partial(sweep_kernel, places),
        grid=(2,),
        in_specs=[pl.BlockSpec(memory_space=pltpu.SMEM)] + [per_species(a) for a in blocked],
        out_specs=per_species(sections),
        out_shape=jax.ShapeDtypeStruct(sections.shape, jnp.float32),
        scratch_shapes=[pltpu.VMEM((total, columns), jnp.float32)] * 3,
        compiler_params=pltpu.CompilerParams(vmem_limit_bytes=32 * 2**20),
    )(factors, *blocked)


def shifted(array, axis, outer, inner, by_outer, by_inner):
    pairs = []
    for i in range(outer):
        for j in range(inner):
            target = ((i + by_outer) % outer) * inner + (j + by_inner) % inner
            pairs.append((i * inner + j, target))
    return lax.ppermute(array, axis, pairs)


def factored(total):
    inner = next(b for b in range(1, total + 1) if total % b == 0 and b * b >= total)
    return total // inner, inner


def exchange_tables(total, quad):
    outer, inner = factored(total)
    node = np.arange(total)
    high, low = node // inner, node % inner
    index = lambda i, j: (i % outer) * inner + j % inner
    table_u = np.zeros((total, outer, inner))
    table_v = np.zeros((total, inner, outer))
    for s in range(outer):
        for g in range(inner):
            table_u[:, s, g] = quad[index(high + s, low), index(high, low - g)]
            table_v[:, g, s] = quad[index(high, low + g), index(high - s, low)]
    return step_size * np.concatenate([table_u.reshape(total, -1), table_v.reshape(total, -1)], 1)


def combined(weights, fields):
    value = weights[0] * fields[0]
    for weight, field in zip(weights[1:], fields[1:]):
        value = value + weight * field
    return value


def shards(initial, sections, feed_rate, kill_rate):
    own = sections[0]
    _, rows, columns = own.shape
    nodes = lax.axis_size("node")
    spaces = lax.axis_size("space")
    outer, inner = factored(nodes)
    points, quad = radau_table(nodes)
    coupling = step_size * points[:, None] * np.array(diffusion)[None]
    divisor = 4.0 * coupling + 1.0
    constants = np.concatenate(
        [exchange_tables(nodes, quad), 1.0 / divisor, coupling / divisor], axis=1
    ).astype(np.float32)
    mine = lax.dynamic_index_in_dim(jnp.asarray(constants), lax.axis_index("node"), 0, False)
    weights_u = mine[:nodes].reshape(outer, inner)
    weights_v = mine[nodes : 2 * nodes].reshape(inner, outer)
    factors = mine[2 * nodes :].reshape(2, 2)

    upward = [(i, (i + 1) % spaces) for i in range(spaces)]
    downward = [(j, i) for i, j in upward]
    before = lax.ppermute(own[:, rows - 1 :], "space", upward)
    after = lax.ppermute(own[:, :1], "space", downward)

    edges = (0, rows - TILE)
    middle = list(range(TILE, rows - TILE, TILE))
    half = (len(middle) + 1) // 2
    lead, rest = tuple(middle[:half]), tuple(middle[half:])
    places = (lead, edges, rest)

    slopes = [None] * 3
    slopes[0] = slopes_of((lead,), (), own, feed_rate, kill_rate)
    out = slopes_of((edges, rest), (before, after), own, feed_rate, kill_rate)
    slopes[1], slopes[2] = out[:2], out[2:]

    along_inner = lambda a, s: shifted(a, "node", outer, inner, 0, s)
    along_outer = lambda a, s: shifted(a, "node", outer, inner, s, 0)

    gathered = []
    for u, v in slopes:
        fields_u = [u] + [along_inner(u, s) for s in range(1, inner)]
        fields_v = [v] + [along_outer(v, s) for s in range(1, outer)]
        gathered.append((fields_u, fields_v))

    arrived = []
    for fields_u, fields_v in gathered:
        sums_u = [along_outer(combined(weights_u[s], fields_u), s) for s in range(1, outer)]
        sums_v = [along_inner(combined(weights_v[s], fields_v), s) for s in range(1, inner)]
        arrived.append((sums_u, sums_v))

    def cut(array, starts):
        parts = []
        for start in starts:
            if parts and parts[-1][1] == start:
                parts[-1][1] = start + TILE
            else:
                parts.append([start, start + TILE])
        cuts = [array[:, a:b] for a, b in parts]
        return cuts[0] if len(cuts) == 1 else jnp.concatenate(cuts, axis=1)

    residuals = []
    for starts, (fields_u, fields_v), (sums_u, sums_v) in zip(places, gathered, arrived):
        total_u = combined(weights_u[0], fields_u) + sum(sums_u)
        total_v = combined(weights_v[0], fields_v) + sum(sums_v)
        local = cut(initial, starts) - cut(own, starts)
        residuals.append(local + jnp.stack([total_u, total_v]))

    edge = residuals[1]
    low_edge = lax.ppermute(edge[:, TILE:], "space", upward)
    high_edge = lax.ppermute(edge[:, :TILE], "space", downward)

    largest = jnp.max(jnp.stack([jnp.max(jnp.abs(r)) for r in residuals]))
    largest = jnp.full((8, 128), largest)
    for axis in ("node", "space"):
        size = lax.axis_size(axis)
        others = [
            lax.ppermute(largest, axis, [(i, (i + s) % size) for i in range(size)])
            for s in range(1, size)
        ]
        for other in others:
            largest = jnp.maximum(largest, other)
    new = swept(places, factors, low_edge, high_edge, own, residuals)
    return new[None], largest[0, 0]


def solution(mesh):
    placed = (
        P(None, "space", None),
        P("node", None, "space", None),
        P("space", None),
        P("space", None),
    )
    return jax.shard_map(
        shards,
        mesh=mesh,
        in_specs=placed,
        out_specs=(P("node", None, "space", None), P()),
        check_vma=False,
    )
```

```python
from functools import partial

import jax
import jax.numpy as jnp
import numpy as np
from jax import lax
from jax.experimental import pallas as pl
from jax.experimental.pallas import tpu as pltpu
from jax.sharding import PartitionSpec as P

SWEEPS = 6
TILE = 8

step_size = 4.0
diffusion = (1.0, 0.5)


def radau_target(order, value):
    before = 1.0
    current = value
    previous = 1.0
    for degree in range(1, order):
        following = ((2 * degree + 1) * value * current - degree * before) / (degree + 1)
        before = current
        current = following
    previous = before
    return current - previous


def radau_table(total):
    grid_count = 20000
    roots_found = []
    left_value = -1.0
    left_target = radau_target(total, left_value)
    for step_index in range(1, grid_count):
        right_value = -1.0 + 2.0 * step_index / grid_count
        right_target = radau_target(total, right_value)
        if left_target * right_target < 0.0:
            lower = left_value
            upper = right_value
            lower_target = left_target
            for bisect_index in range(80):
                halfway = 0.5 * (lower + upper)
                halfway_target = radau_target(total, halfway)
                if lower_target * halfway_target <= 0.0:
                    upper = halfway
                else:
                    lower = halfway
                    lower_target = halfway_target
            roots_found.append(0.5 * (lower + upper))
        left_value = right_value
        left_target = right_target
    roots_found.append(1.0)
    points = [(value + 1.0) / 2.0 for value in roots_found]
    quad_rows = []
    for node_index in range(total):
        row_values = []
        for basis_index in range(total):
            coefs = [1.0]
            for other_index in range(total):
                if other_index != basis_index:
                    scale = 1.0 / (points[basis_index] - points[other_index])
                    shifted = [0.0] + coefs
                    widened = coefs + [0.0]
                    coefs = [
                        (shifted[k] - points[other_index] * widened[k]) * scale
                        for k in range(len(shifted))
                    ]
            integral = 0.0
            for power_index in range(len(coefs)):
                integral += (
                    coefs[power_index] * points[node_index] ** (power_index + 1) / (power_index + 1)
                )
            row_values.append(integral)
        quad_rows.append(row_values)
    return (np.array(points), np.array(quad_rows))


LANES = 128


def by_node(values):
    values = [float(np.float32(v)) for v in values]
    node = lax.axis_index("node")
    result = jnp.float32(values[0])
    for k, value in enumerate(values[1:], 1):
        result = jnp.where(node == k, jnp.float32(value), result)
    return result


def neighbour_sum(above, tile, below):
    rows, columns = tile.shape
    row = lax.broadcasted_iota(jnp.int32, tile.shape, 0)
    up = jnp.where(row == 0, above, pltpu.roll(tile, 1, 0))
    down = jnp.where(row == rows - 1, below, pltpu.roll(tile, rows - 1, 0))
    return (up + down) + (pltpu.roll(tile, 1, 1) + pltpu.roll(tile, columns - 1, 1))


def tile_slopes(u_rows, v_rows, feed, kill):
    above_u, u, below_u = u_rows
    above_v, v, below_v = v_rows
    product = u * v * v
    slope_u = diffusion[0] * (neighbour_sum(above_u, u, below_u) - 4.0 * u)
    slope_v = diffusion[1] * (neighbour_sum(above_v, v, below_v) - 4.0 * v)
    slope_u = slope_u + (feed * (1.0 - u) - product)
    slope_v = slope_v + (product - (feed + kill) * v)
    return slope_u, slope_v


def rows_of(ref, species, start, before, after):
    length = ref.shape[1]
    above = before[species] if start == 0 else ref[species, start - 1 : start]
    stop = start + TILE
    below = after[species] if stop == length else ref[species, stop : stop + 1]
    return above, ref[species, start:stop], below


def lead_kernel(starts, sections, feed, kill, out_u, out_v, first, last, w, f, k, tail, sems):
    low, high = starts[0], starts[-1] + TILE
    rows = sections.shape[1]
    copies = [
        pltpu.make_async_copy(sections.at[:, 0 : high + TILE], w, sems.at[0]),
        pltpu.make_async_copy(feed.at[low:high], f, sems.at[1]),
        pltpu.make_async_copy(kill.at[low:high], k, sems.at[2]),
        pltpu.make_async_copy(sections.at[:, rows - TILE : rows], tail, sems.at[3]),
    ]
    for copy in copies:
        copy.start()
    for copy in copies:
        copy.wait()
    for n, start in enumerate(starts):
        here = slice(n * TILE, (n + 1) * TILE)
        slope_u, slope_v = tile_slopes(
            rows_of(w, 0, start, None, None), rows_of(w, 1, start, None, None), f[here], k[here]
        )
        out_u[here] = slope_u
        out_v[here] = slope_v
    first[...] = w[:, 0:1]
    last[...] = tail[:, TILE - 1 : TILE]


def lead_slopes(starts, sections, feed_rate, kill_rate):
    columns = sections.shape[-1]
    count = len(starts) * TILE
    shape = lambda *s: jax.ShapeDtypeStruct(s, jnp.float32)
    return pl.pallas_call(
        partial(lead_kernel, starts),
        in_specs=[pl.BlockSpec(memory_space=pltpu.HBM)] * 3,
        out_shape=[shape(count, columns)] * 2 + [shape(2, 1, columns)] * 2,
        scratch_shapes=[
            pltpu.VMEM((2, starts[-1] + 2 * TILE, columns), jnp.float32),
            pltpu.VMEM((count, columns), jnp.float32),
            pltpu.VMEM((count, columns), jnp.float32),
            pltpu.VMEM((2, TILE, columns), jnp.float32),
            pltpu.SemaphoreType.DMA((4,)),
        ],
        compiler_params=pltpu.CompilerParams(vmem_limit_bytes=12 * 2**20),
    )(sections, feed_rate, kill_rate)


def slopes_kernel(groups, before, after, sections, feed, kill, *outs):
    for group, starts in enumerate(groups):
        for k, start in enumerate(starts):
            slope_u, slope_v = tile_slopes(
                rows_of(sections, 0, start, before, after),
                rows_of(sections, 1, start, before, after),
                feed[start : start + TILE],
                kill[start : start + TILE],
            )
            outs[2 * group][k * TILE : (k + 1) * TILE] = slope_u
            outs[2 * group + 1][k * TILE : (k + 1) * TILE] = slope_v


def slopes_of(groups, before, after, sections, feed_rate, kill_rate):
    columns = sections.shape[-1]
    shapes = []
    for starts in groups:
        shapes += [jax.ShapeDtypeStruct((len(starts) * TILE, columns), jnp.float32)] * 2
    return pl.pallas_call(
        partial(slopes_kernel, groups),
        out_shape=shapes,
        compiler_params=pltpu.CompilerParams(vmem_limit_bytes=16 * 2**20),
    )(before, after, sections, feed_rate, kill_rate)


def combined(weights, fields):
    value = weights[0] * fields[0]
    for weight, field in zip(weights[1:], fields[1:]):
        value = value + weight * field
    return value


def tiles(ref):
    return [slice(k, k + TILE) for k in range(0, ref.shape[-2], TILE)]


def message_kernel(tables, counts, *refs):
    refs = list(refs)
    fields = [[refs.pop(0) for _ in range(count)] for count in counts]
    for table, sources in zip(tables, fields):
        for s in range(1, table.shape[1]):
            out = refs.pop(0)
            weights = [by_node(table[:, s, g]) for g in range(len(sources))]
            for here in tiles(out):
                out[here] = combined(weights, [source[here] for source in sources])


def messages(tables, fields):
    counts = tuple(len(f) for f in fields)
    number = sum(table.shape[1] - 1 for table in tables)
    like = fields[0][0]
    return pl.pallas_call(
        partial(message_kernel, tables, counts),
        out_shape=[jax.ShapeDtypeStruct(like.shape, like.dtype)] * number,
        compiler_params=pltpu.CompilerParams(vmem_limit_bytes=12 * 2**20),
    )(*fields[0], *fields[1])


def local_kernel(tables, counts, starts, initial, sections, *refs):
    refs = list(refs)
    fields = [[refs.pop(0) for _ in range(count)] for count in counts]
    (out,) = refs
    for species in range(2):
        sources = fields[species]
        weights = [by_node(tables[species][:, 0, g]) for g in range(len(sources))]
        for start, here in zip(starts, tiles(out)):
            there = slice(start, start + TILE)
            difference = initial[species, there] - sections[species, there]
            out[species, here] = difference + combined(weights, [f[here] for f in sources])


def local_part(tables, starts, initial, sections, fields):
    counts = tuple(len(f) for f in fields)
    like = fields[0][0]
    return pl.pallas_call(
        partial(local_kernel, tables, counts, starts),
        out_shape=jax.ShapeDtypeStruct((2,) + like.shape, like.dtype),
        compiler_params=pltpu.CompilerParams(vmem_limit_bytes=16 * 2**20),
    )(initial, sections, *fields[0], *fields[1])


def residual_kernel(counts, split, local, *refs):
    refs = list(refs)
    sums = [[refs.pop(0) for _ in range(count)] for count in counts]
    largest = refs.pop()
    top = jnp.zeros((TILE, LANES), jnp.float32)
    columns = local.shape[-1]
    for species in range(2):
        for n, here in enumerate(tiles(local)):
            for c in range(0, columns, LANES):
                block = (here, slice(c, c + LANES))
                value = local[(species,) + block]
                for part in sums[species]:
                    value = value + part[block]
                if split:
                    refs[n][species, :, c : c + LANES] = value
                else:
                    refs[0][(species,) + block] = value
                top = jnp.maximum(top, jnp.abs(value))
    largest[...] = top


def residual_of(local, sums, split):
    counts = tuple(len(s) for s in sums)
    _, rows, columns = local.shape
    pieces = rows // TILE if split else 1
    shape = lambda *s: jax.ShapeDtypeStruct(s, jnp.float32)
    return pl.pallas_call(
        partial(residual_kernel, counts, split),
        out_shape=[shape(2, rows // pieces, columns)] * pieces + [shape(TILE, LANES)],
        compiler_params=pltpu.CompilerParams(vmem_limit_bytes=12 * 2**20),
    )(local, *sums[0], *sums[1])


def sweep_kernel(species, places, table, before, after, sections, *refs):
    pieces = refs[: len(places)]
    out, first, even, odd, result, sems = refs[-6:]
    inverse = by_node(1.0 / (4.0 * table[:, species] + 1.0))
    gain = by_node(table[:, species] / (4.0 * table[:, species] + 1.0))
    total, columns = first.shape
    first[0:TILE] = before[species] * inverse
    first[total - TILE : total] = after[species] * inverse
    for piece, starts in zip(pieces, places):
        for k, start in enumerate(starts):
            scaled = piece[species, k * TILE : (k + 1) * TILE] * inverse
            first[start + TILE : start + 2 * TILE] = scaled

    row = lax.broadcasted_iota(jnp.int32, (TILE, LANES), 0)
    lane = lax.broadcasted_iota(jnp.int32, (TILE, LANES), 1)
    blocks = columns // LANES

    def update(source, start, store):
        above_at = pl.ds(pl.multiple_of(jnp.maximum(start - TILE, 0), TILE), TILE)
        below_at = pl.ds(pl.multiple_of(jnp.minimum(start + TILE, total - TILE), TILE), TILE)
        here = pl.ds(start, TILE)
        cut = lambda b: slice((b % blocks) * LANES, (b % blocks + 1) * LANES)
        load = lambda b: source[here, cut(b)]
        right = lambda x: pltpu.roll(x, 1, 1)
        left = lambda x: pltpu.roll(x, LANES - 1, 1)
        tile, following = load(0), load(1)
        tile_left = left(tile)
        before_right = right(load(blocks - 1))
        for b in range(blocks):
            tile_right = right(tile)
            following_left = left(following)
            west = jnp.where(lane == 0, before_right, tile_right)
            east = jnp.where(lane == LANES - 1, following_left, tile_left)
            up = pltpu.roll(jnp.where(row == TILE - 1, source[above_at, cut(b)], tile), 1, 0)
            down = pltpu.roll(jnp.where(row == 0, source[below_at, cut(b)], tile), TILE - 1, 0)
            store(cut(b), first[here, cut(b)] + gain * ((up + down) + (west + east)))
            before_right, tile, tile_left = tile_right, following, following_left
            following = load(b + 2)

    source = first
    for sweep in range(SWEEPS - 2):
        target = (even, odd)[sweep % 2]

        def one_tile(t, _, source=source, target=target):
            start = pl.multiple_of(t * TILE, TILE)

            def store(at, value):
                target[pl.ds(start, TILE), at] = value

            update(source, start, store)
            return 0

        lax.fori_loop(0, total // TILE, one_tile, 0)
        source = target

    def last_tile(t, _):
        start = pl.multiple_of(t * TILE, TILE)

        def store(at, value):
            result[pl.ds(start, TILE), at] = sections[species, pl.ds(start, TILE), at] + value

        update(source, pl.multiple_of(start + TILE, TILE), store)
        return 0

    count = total // TILE - 2
    bounds = (0, count // 2, count)
    copies = []
    for part in range(2):
        lax.fori_loop(bounds[part], bounds[part + 1], last_tile, 0)
        span = slice(bounds[part] * TILE, bounds[part + 1] * TILE)
        copies.append(
            pltpu.make_async_copy(result.at[span], out.at[species, span], sems.at[part])
        )
        copies[-1].start()
    for copy in copies:
        copy.wait()


def swept(species, places, table, before, after, sections, pieces, out):
    _, rows, columns = sections.shape
    total = rows + 2 * TILE
    operands = [before, after, sections, *pieces]
    specs = [pl.BlockSpec(memory_space=pltpu.VMEM)] * len(operands)
    aliases = {}
    if out is not None:
        aliases = {len(operands): 0}
        operands.append(out)
        specs.append(pl.BlockSpec(memory_space=pltpu.HBM))
    return pl.pallas_call(
        partial(sweep_kernel, species, places, table),
        in_specs=specs,
        out_specs=pl.BlockSpec(memory_space=pltpu.HBM),
        out_shape=jax.ShapeDtypeStruct(sections.shape, jnp.float32),
        input_output_aliases=aliases,
        scratch_shapes=[pltpu.VMEM((total, columns), jnp.float32)] * 3
        + [pltpu.VMEM((rows, columns), jnp.float32), pltpu.SemaphoreType.DMA((2,))],
        compiler_params=pltpu.CompilerParams(vmem_limit_bytes=20 * 2**20),
    )(*operands)


def shifted(array, axis, outer, inner, by_outer, by_inner):
    pairs = []
    for i in range(outer):
        for j in range(inner):
            target = ((i + by_outer) % outer) * inner + (j + by_inner) % inner
            pairs.append((i * inner + j, target))
    return lax.ppermute(array, axis, pairs)


def factored(total):
    inner = next(b for b in range(1, total + 1) if total % b == 0 and b * b >= total)
    return total // inner, inner


def exchange_tables(total, quad):
    outer, inner = factored(total)
    node = np.arange(total)
    high, low = node // inner, node % inner
    index = lambda i, j: (i % outer) * inner + j % inner
    table_u = np.zeros((total, outer, inner))
    table_v = np.zeros((total, inner, outer))
    for s in range(outer):
        for g in range(inner):
            table_u[:, s, g] = quad[index(high + s, low), index(high, low - g)]
            table_v[:, g, s] = quad[index(high, low + g), index(high - s, low)]
    return step_size * table_u, step_size * table_v


def spread_rounds(size):
    covered = 1
    while covered < size:
        shifts = [s * covered for s in (1, 2, 3) if s * covered < size]
        yield shifts
        covered *= len(shifts) + 1


def shards(initial, sections, feed_rate, kill_rate):
    own = sections[0]
    _, rows, columns = own.shape
    nodes = lax.axis_size("node")
    spaces = lax.axis_size("space")
    outer, inner = factored(nodes)
    points, quad = radau_table(nodes)
    coupling = step_size * points[:, None] * np.array(diffusion)[None]
    tables = exchange_tables(nodes, quad)

    edges = (0, rows - TILE)
    middle = list(range(TILE, rows - TILE, TILE))
    half = (len(middle) + 1) // 2
    lead, rest = tuple(middle[:half]), tuple(middle[half:])
    places = (lead, edges, rest)

    along_inner = lambda a, s: shifted(a, "node", outer, inner, 0, s)
    along_outer = lambda a, s: shifted(a, "node", outer, inner, s, 0)

    def gather(u, v):
        fields_u = [u] + [along_inner(u, s) for s in range(1, inner)]
        fields_v = [v] + [along_outer(v, s) for s in range(1, outer)]
        return fields_u, fields_v

    def exchange(fields):
        sent = messages(tables, fields)
        sums_u = [along_outer(sent[s - 1], s) for s in range(1, outer)]
        sums_v = [along_inner(sent[outer - 2 + s], s) for s in range(1, inner)]
        return sums_u, sums_v

    upward = [(i, (i + 1) % spaces) for i in range(spaces)]
    downward = [(j, i) for i, j in upward]
    lead_u, lead_v, first, last = lead_slopes(lead, own, feed_rate, kill_rate)
    gathered = [gather(lead_u, lead_v)]
    before = lax.ppermute(last, "space", upward)
    after = lax.ppermute(first, "space", downward)
    out = slopes_of((edges, rest), before, after, own, feed_rate, kill_rate)
    gathered += [gather(*out[:2]), gather(*out[2:])]
    sums = [exchange(fields) for fields in gathered]
    local = [
        local_part(tables, starts, initial, own, fields)
        for starts, fields in zip(places, gathered)
    ]

    low, high, edge_largest = residual_of(local[1], sums[1], True)
    low_edge = lax.ppermute(high, "space", upward)
    high_edge = lax.ppermute(low, "space", downward)
    lead_residual, lead_largest = residual_of(local[0], sums[0], False)
    low_edge, high_edge, lead_largest, edge_largest, last_sums = lax.optimization_barrier(
        (low_edge, high_edge, lead_largest, edge_largest, sums[2])
    )
    rest_residual, rest_largest = residual_of(local[2], last_sums, False)
    largest = jnp.maximum(jnp.maximum(lead_largest, edge_largest), rest_largest)
    largest = jnp.broadcast_to(jnp.max(largest), (TILE, LANES))

    def spread(value, axis):
        size = lax.axis_size(axis)
        for shifts in spread_rounds(size):
            others = [
                lax.ppermute(value, axis, [(i, (i + s) % size) for i in range(size)])
                for s in shifts
            ]
            for other in others:
                value = jnp.maximum(value, other)
        return value

    pieces = [lead_residual, low, high, rest_residual]
    spots = (lead, edges[:1], edges[1:], rest)
    largest = spread(largest, "node")
    new = swept(0, spots, coupling, low_edge, high_edge, own, pieces, None)
    largest, new = lax.optimization_barrier((largest, new))
    new = swept(1, spots, coupling, low_edge, high_edge, own, pieces, new)
    largest = spread(largest, "space")
    return new[None], largest[0, 0]


def solution(mesh):
    placed = (
        P(None, "space", None),
        P("node", None, "space", None),
        P("space", None),
        P("space", None),
    )
    return jax.shard_map(
        shards,
        mesh=mesh,
        in_specs=placed,
        out_specs=(P("node", None, "space", None), P()),
        check_vma=False,
    )
```

```python
from functools import partial

import jax
import jax.numpy as jnp
import numpy as np
from jax import lax
from jax.experimental import pallas as pl
from jax.experimental.pallas import tpu as pltpu
from jax.sharding import PartitionSpec as P

SWEEPS = 6
TILE = 8

step_size = 4.0
diffusion = (1.0, 0.5)


def radau_target(order, value):
    before = 1.0
    current = value
    previous = 1.0
    for degree in range(1, order):
        following = ((2 * degree + 1) * value * current - degree * before) / (degree + 1)
        before = current
        current = following
    previous = before
    return current - previous


def radau_table(total):
    grid_count = 20000
    roots_found = []
    left_value = -1.0
    left_target = radau_target(total, left_value)
    for step_index in range(1, grid_count):
        right_value = -1.0 + 2.0 * step_index / grid_count
        right_target = radau_target(total, right_value)
        if left_target * right_target < 0.0:
            lower = left_value
            upper = right_value
            lower_target = left_target
            for bisect_index in range(80):
                halfway = 0.5 * (lower + upper)
                halfway_target = radau_target(total, halfway)
                if lower_target * halfway_target <= 0.0:
                    upper = halfway
                else:
                    lower = halfway
                    lower_target = halfway_target
            roots_found.append(0.5 * (lower + upper))
        left_value = right_value
        left_target = right_target
    roots_found.append(1.0)
    points = [(value + 1.0) / 2.0 for value in roots_found]
    quad_rows = []
    for node_index in range(total):
        row_values = []
        for basis_index in range(total):
            coefs = [1.0]
            for other_index in range(total):
                if other_index != basis_index:
                    scale = 1.0 / (points[basis_index] - points[other_index])
                    shifted = [0.0] + coefs
                    widened = coefs + [0.0]
                    coefs = [
                        (shifted[k] - points[other_index] * widened[k]) * scale
                        for k in range(len(shifted))
                    ]
            integral = 0.0
            for power_index in range(len(coefs)):
                integral += (
                    coefs[power_index] * points[node_index] ** (power_index + 1) / (power_index + 1)
                )
            row_values.append(integral)
        quad_rows.append(row_values)
    return (np.array(points), np.array(quad_rows))


LANES = 128
LEAD_LIMIT = 60 * 2**20


def by_node(values):
    values = [float(np.float32(v)) for v in values]
    node = lax.axis_index("node")
    result = jnp.float32(values[0])
    for k, value in enumerate(values[1:], 1):
        result = jnp.where(node == k, jnp.float32(value), result)
    return result


def neighbour_sum(above, tile, below):
    rows, columns = tile.shape
    row = lax.broadcasted_iota(jnp.int32, tile.shape, 0)
    up = jnp.where(row == 0, above, pltpu.roll(tile, 1, 0))
    down = jnp.where(row == rows - 1, below, pltpu.roll(tile, rows - 1, 0))
    return (up + down) + (pltpu.roll(tile, 1, 1) + pltpu.roll(tile, columns - 1, 1))


def tile_slopes(u_rows, v_rows, feed, kill):
    above_u, u, below_u = u_rows
    above_v, v, below_v = v_rows
    product = u * v * v
    slope_u = diffusion[0] * (neighbour_sum(above_u, u, below_u) - 4.0 * u)
    slope_v = diffusion[1] * (neighbour_sum(above_v, v, below_v) - 4.0 * v)
    slope_u = slope_u + (feed * (1.0 - u) - product)
    slope_v = slope_v + (product - (feed + kill) * v)
    return slope_u, slope_v


def rows_of(ref, species, start, before, after):
    length = ref.shape[1]
    above = before[species] if start == 0 else ref[species, start - 1 : start]
    stop = start + TILE
    below = after[species] if stop == length else ref[species, stop : stop + 1]
    return above, ref[species, start:stop], below


def lead_kernel(starts, sections, feed, kill, out_u, out_v, first, last, w, f, k, tail, sems):
    low, high = starts[0], starts[-1] + TILE
    rows = sections.shape[1]
    copies = [
        pltpu.make_async_copy(sections.at[:, 0 : high + TILE], w, sems.at[0]),
        pltpu.make_async_copy(feed.at[low:high], f, sems.at[1]),
        pltpu.make_async_copy(kill.at[low:high], k, sems.at[2]),
        pltpu.make_async_copy(sections.at[:, rows - TILE : rows], tail, sems.at[3]),
    ]
    for copy in copies:
        copy.start()
    for copy in copies:
        copy.wait()
    for n, start in enumerate(starts):
        here = slice(n * TILE, (n + 1) * TILE)
        slope_u, slope_v = tile_slopes(
            rows_of(w, 0, start, None, None), rows_of(w, 1, start, None, None), f[here], k[here]
        )
        out_u[here] = slope_u
        out_v[here] = slope_v
    first[...] = w[:, 0:1]
    last[...] = tail[:, TILE - 1 : TILE]


def lead_slopes(starts, sections, feed_rate, kill_rate):
    columns = sections.shape[-1]
    count = len(starts) * TILE
    shape = lambda *s: jax.ShapeDtypeStruct(s, jnp.float32)
    return pl.pallas_call(
        partial(lead_kernel, starts),
        in_specs=[pl.BlockSpec(memory_space=pltpu.HBM)] * 3,
        out_shape=[shape(count, columns)] * 2 + [shape(2, 1, columns)] * 2,
        scratch_shapes=[
            pltpu.VMEM((2, starts[-1] + 2 * TILE, columns), jnp.float32),
            pltpu.VMEM((count, columns), jnp.float32),
            pltpu.VMEM((count, columns), jnp.float32),
            pltpu.VMEM((2, TILE, columns), jnp.float32),
            pltpu.SemaphoreType.DMA((4,)),
        ],
        compiler_params=pltpu.CompilerParams(vmem_limit_bytes=LEAD_LIMIT),
    )(sections, feed_rate, kill_rate)


def slopes_kernel(groups, before, after, sections, feed, kill, *outs):
    for group, starts in enumerate(groups):
        for k, start in enumerate(starts):
            slope_u, slope_v = tile_slopes(
                rows_of(sections, 0, start, before, after),
                rows_of(sections, 1, start, before, after),
                feed[start : start + TILE],
                kill[start : start + TILE],
            )
            outs[2 * group][k * TILE : (k + 1) * TILE] = slope_u
            outs[2 * group + 1][k * TILE : (k + 1) * TILE] = slope_v


def slopes_of(groups, before, after, sections, feed_rate, kill_rate):
    columns = sections.shape[-1]
    shapes = []
    for starts in groups:
        shapes += [jax.ShapeDtypeStruct((len(starts) * TILE, columns), jnp.float32)] * 2
    return pl.pallas_call(
        partial(slopes_kernel, groups),
        out_shape=shapes,
        compiler_params=pltpu.CompilerParams(vmem_limit_bytes=16 * 2**20),
    )(before, after, sections, feed_rate, kill_rate)


def combined(weights, fields):
    value = weights[0] * fields[0]
    for weight, field in zip(weights[1:], fields[1:]):
        value = value + weight * field
    return value


def tiles(ref):
    return [slice(k, k + TILE) for k in range(0, ref.shape[-2], TILE)]


def message_kernel(tables, counts, *refs):
    refs = list(refs)
    fields = [[refs.pop(0) for _ in range(count)] for count in counts]
    for table, sources in zip(tables, fields):
        for s in range(1, table.shape[1]):
            out = refs.pop(0)
            weights = [by_node(table[:, s, g]) for g in range(len(sources))]
            for here in tiles(out):
                out[here] = combined(weights, [source[here] for source in sources])


def messages(tables, fields):
    counts = tuple(len(f) for f in fields)
    number = sum(table.shape[1] - 1 for table in tables)
    like = fields[0][0]
    return pl.pallas_call(
        partial(message_kernel, tables, counts),
        out_shape=[jax.ShapeDtypeStruct(like.shape, like.dtype)] * number,
        compiler_params=pltpu.CompilerParams(vmem_limit_bytes=12 * 2**20),
    )(*fields[0], *fields[1])


def local_kernel(tables, counts, starts, initial, sections, *refs):
    refs = list(refs)
    fields = [[refs.pop(0) for _ in range(count)] for count in counts]
    (out,) = refs
    for species in range(2):
        sources = fields[species]
        weights = [by_node(tables[species][:, 0, g]) for g in range(len(sources))]
        for start, here in zip(starts, tiles(out)):
            there = slice(start, start + TILE)
            difference = initial[species, there] - sections[species, there]
            out[species, here] = difference + combined(weights, [f[here] for f in sources])


def local_part(tables, starts, initial, sections, fields):
    counts = tuple(len(f) for f in fields)
    like = fields[0][0]
    return pl.pallas_call(
        partial(local_kernel, tables, counts, starts),
        out_shape=jax.ShapeDtypeStruct((2,) + like.shape, like.dtype),
        compiler_params=pltpu.CompilerParams(vmem_limit_bytes=16 * 2**20),
    )(initial, sections, *fields[0], *fields[1])


def residual_kernel(counts, split, maxima, local, *refs):
    refs = list(refs)
    earlier = [refs.pop(0) for _ in range(maxima)]
    sums = [[refs.pop(0) for _ in range(count)] for count in counts]
    largest = refs.pop()
    top = jnp.zeros((TILE, LANES), jnp.float32)
    for ref in earlier:
        top = jnp.maximum(top, ref[...])
    columns = local.shape[-1]
    for species in range(2):
        for n, here in enumerate(tiles(local)):
            for c in range(0, columns, LANES):
                block = (here, slice(c, c + LANES))
                value = local[(species,) + block]
                for part in sums[species]:
                    value = value + part[block]
                if split:
                    refs[n][species, :, c : c + LANES] = value
                else:
                    refs[0][(species,) + block] = value
                top = jnp.maximum(top, jnp.abs(value))
    largest[...] = top


def residual_of(local, sums, split, earlier=()):
    counts = tuple(len(s) for s in sums)
    _, rows, columns = local.shape
    pieces = rows // TILE if split else 1
    shape = lambda *s: jax.ShapeDtypeStruct(s, jnp.float32)
    return pl.pallas_call(
        partial(residual_kernel, counts, split, len(earlier)),
        out_shape=[shape(2, rows // pieces, columns)] * pieces + [shape(TILE, LANES)],
        compiler_params=pltpu.CompilerParams(vmem_limit_bytes=12 * 2**20),
    )(local, *earlier, *sums[0], *sums[1])


def sweep_kernel(species, places, table, before, after, sections, *refs):
    pieces = refs[: len(places)]
    out, first, even, odd, result, sems = refs[-6:]
    inverse = by_node(1.0 / (4.0 * table[:, species] + 1.0))
    gain = by_node(table[:, species] / (4.0 * table[:, species] + 1.0))
    total, columns = first.shape
    first[0:TILE] = before[species] * inverse
    first[total - TILE : total] = after[species] * inverse
    for piece, starts in zip(pieces, places):
        for k, start in enumerate(starts):
            scaled = piece[species, k * TILE : (k + 1) * TILE] * inverse
            first[start + TILE : start + 2 * TILE] = scaled

    row = lax.broadcasted_iota(jnp.int32, (TILE, LANES), 0)
    lane = lax.broadcasted_iota(jnp.int32, (TILE, LANES), 1)
    blocks = columns // LANES

    def update(source, start, store):
        above_at = pl.ds(pl.multiple_of(jnp.maximum(start - TILE, 0), TILE), TILE)
        below_at = pl.ds(pl.multiple_of(jnp.minimum(start + TILE, total - TILE), TILE), TILE)
        here = pl.ds(start, TILE)
        cut = lambda b: slice((b % blocks) * LANES, (b % blocks + 1) * LANES)
        load = lambda b: source[here, cut(b)]
        right = lambda x: pltpu.roll(x, 1, 1)
        left = lambda x: pltpu.roll(x, LANES - 1, 1)
        tile, following = load(0), load(1)
        tile_left = left(tile)
        before_right = right(load(blocks - 1))
        for b in range(blocks):
            tile_right = right(tile)
            following_left = left(following)
            west = jnp.where(lane == 0, before_right, tile_right)
            east = jnp.where(lane == LANES - 1, following_left, tile_left)
            up = pltpu.roll(jnp.where(row == TILE - 1, source[above_at, cut(b)], tile), 1, 0)
            down = pltpu.roll(jnp.where(row == 0, source[below_at, cut(b)], tile), TILE - 1, 0)
            store(cut(b), first[here, cut(b)] + gain * ((up + down) + (west + east)))
            before_right, tile, tile_left = tile_right, following, following_left
            following = load(b + 2)

    source = first
    for sweep in range(SWEEPS - 2):
        target = (even, odd)[sweep % 2]

        def one_tile(t, _, source=source, target=target):
            start = pl.multiple_of(t * TILE, TILE)

            def store(at, value):
                target[pl.ds(start, TILE), at] = value

            update(source, start, store)
            return 0

        lax.fori_loop(0, total // TILE, one_tile, 0, unroll=5)
        source = target

    def last_tile(t, _):
        start = pl.multiple_of(t * TILE, TILE)

        def store(at, value):
            result[pl.ds(start, TILE), at] = sections[species, pl.ds(start, TILE), at] + value

        update(source, pl.multiple_of(start + TILE, TILE), store)
        return 0

    count = total // TILE - 2
    bounds = (0, count // 2, count)
    copies = []
    for part in range(2):
        lax.fori_loop(bounds[part], bounds[part + 1], last_tile, 0, unroll=4)
        span = slice(bounds[part] * TILE, bounds[part + 1] * TILE)
        copies.append(
            pltpu.make_async_copy(result.at[span], out.at[species, span], sems.at[part])
        )
        copies[-1].start()
    for copy in copies:
        copy.wait()


def swept(species, places, table, before, after, sections, pieces, out):
    _, rows, columns = sections.shape
    total = rows + 2 * TILE
    operands = [before, after, sections, *pieces]
    specs = [pl.BlockSpec(memory_space=pltpu.VMEM)] * len(operands)
    aliases = {}
    if out is not None:
        aliases = {len(operands): 0}
        operands.append(out)
        specs.append(pl.BlockSpec(memory_space=pltpu.HBM))
    return pl.pallas_call(
        partial(sweep_kernel, species, places, table),
        in_specs=specs,
        out_specs=pl.BlockSpec(memory_space=pltpu.HBM),
        out_shape=jax.ShapeDtypeStruct(sections.shape, jnp.float32),
        input_output_aliases=aliases,
        scratch_shapes=[pltpu.VMEM((total, columns), jnp.float32)] * 3
        + [pltpu.VMEM((rows, columns), jnp.float32), pltpu.SemaphoreType.DMA((2,))],
        compiler_params=pltpu.CompilerParams(vmem_limit_bytes=20 * 2**20),
    )(*operands)


def shifted(array, axis, outer, inner, by_outer, by_inner):
    pairs = []
    for i in range(outer):
        for j in range(inner):
            target = ((i + by_outer) % outer) * inner + (j + by_inner) % inner
            pairs.append((i * inner + j, target))
    return lax.ppermute(array, axis, pairs)


def factored(total):
    inner = next(b for b in range(1, total + 1) if total % b == 0 and b * b >= total)
    return total // inner, inner


def exchange_tables(total, quad):
    outer, inner = factored(total)
    node = np.arange(total)
    high, low = node // inner, node % inner
    index = lambda i, j: (i % outer) * inner + j % inner
    table_u = np.zeros((total, outer, inner))
    table_v = np.zeros((total, inner, outer))
    for s in range(outer):
        for g in range(inner):
            table_u[:, s, g] = quad[index(high + s, low), index(high, low - g)]
            table_v[:, g, s] = quad[index(high, low + g), index(high - s, low)]
    return step_size * table_u, step_size * table_v


def spread_pairs(size, shift):
    if size & (size - 1) == 0:
        return [(i, i ^ shift) for i in range(size)]
    return [(i, (i + shift) % size) for i in range(size)]


def spread_rounds(size):
    covered = 1
    while covered < size:
        shifts = [s * covered for s in (1, 2, 3) if s * covered < size]
        yield shifts
        covered *= len(shifts) + 1


def shards(initial, sections, feed_rate, kill_rate):
    own = sections[0]
    _, rows, columns = own.shape
    nodes = lax.axis_size("node")
    spaces = lax.axis_size("space")
    outer, inner = factored(nodes)
    points, quad = radau_table(nodes)
    coupling = step_size * points[:, None] * np.array(diffusion)[None]
    tables = exchange_tables(nodes, quad)

    edges = (0, rows - TILE)
    middle = list(range(TILE, rows - TILE, TILE))
    half = (len(middle) + 1) // 2
    lead, rest = tuple(middle[:half]), tuple(middle[half:])
    places = (lead, edges, rest)

    along_inner = lambda a, s: shifted(a, "node", outer, inner, 0, s)
    along_outer = lambda a, s: shifted(a, "node", outer, inner, s, 0)

    def gather(u, v):
        fields_u = [u] + [along_inner(u, s) for s in range(1, inner)]
        fields_v = [v] + [along_outer(v, s) for s in range(1, outer)]
        return fields_u, fields_v

    def exchange(fields):
        sent = messages(tables, fields)
        sums_u = [along_outer(sent[s - 1], s) for s in range(1, outer)]
        sums_v = [along_inner(sent[outer - 2 + s], s) for s in range(1, inner)]
        return sums_u, sums_v

    upward = [(i, (i + 1) % spaces) for i in range(spaces)]
    downward = [(j, i) for i, j in upward]
    lead_u, lead_v, first, last = lead_slopes(lead, own, feed_rate, kill_rate)
    gathered = [gather(lead_u, lead_v)]
    before = lax.ppermute(last, "space", upward)
    after = lax.ppermute(first, "space", downward)
    out = slopes_of((edges, rest), before, after, own, feed_rate, kill_rate)
    gathered += [gather(*out[:2]), gather(*out[2:])]
    sums = [exchange(fields) for fields in gathered]
    local = [
        local_part(tables, starts, initial, own, fields)
        for starts, fields in zip(places, gathered)
    ]

    low, high, edge_largest = residual_of(local[1], sums[1], True)
    low_edge = lax.ppermute(high, "space", upward)
    high_edge = lax.ppermute(low, "space", downward)
    lead_residual, lead_largest = residual_of(local[0], sums[0], False)
    low_edge, high_edge, lead_largest, edge_largest, last_sums = lax.optimization_barrier(
        (low_edge, high_edge, lead_largest, edge_largest, sums[2])
    )
    rest_residual, largest = residual_of(
        local[2], last_sums, False, (lead_largest, edge_largest)
    )

    def spread(value, axis):
        size = lax.axis_size(axis)
        for shifts in spread_rounds(size):
            others = [
                lax.ppermute(value, axis, spread_pairs(size, s))
                for s in shifts
            ]
            for other in others:
                value = jnp.maximum(value, other)
        return value

    pieces = [lead_residual, low, high, rest_residual]
    spots = (lead, edges[:1], edges[1:], rest)
    largest = spread(largest, "node")
    new = swept(0, spots, coupling, low_edge, high_edge, own, pieces, None)
    largest, new = lax.optimization_barrier((largest, new))
    new = swept(1, spots, coupling, low_edge, high_edge, own, pieces, new)
    largest = spread(largest, "space")
    return new[None], jnp.max(largest)


def solution(mesh):
    placed = (
        P(None, "space", None),
        P("node", None, "space", None),
        P("space", None),
        P("space", None),
    )
    return jax.shard_map(
        shards,
        mesh=mesh,
        in_specs=placed,
        out_specs=(P("node", None, "space", None), P()),
        check_vma=False,
    )
```

```python
from functools import partial

import jax
import jax.numpy as jnp
import numpy as np
from jax import lax
from jax.experimental import pallas as pl
from jax.experimental.pallas import tpu as pltpu
from jax.sharding import PartitionSpec as P

SWEEPS = 6
TILE = 8

step_size = 4.0
diffusion = (1.0, 0.5)


def radau_target(order, value):
    before = 1.0
    current = value
    previous = 1.0
    for degree in range(1, order):
        following = ((2 * degree + 1) * value * current - degree * before) / (degree + 1)
        before = current
        current = following
    previous = before
    return current - previous


def radau_table(total):
    grid_count = 20000
    roots_found = []
    left_value = -1.0
    left_target = radau_target(total, left_value)
    for step_index in range(1, grid_count):
        right_value = -1.0 + 2.0 * step_index / grid_count
        right_target = radau_target(total, right_value)
        if left_target * right_target < 0.0:
            lower = left_value
            upper = right_value
            lower_target = left_target
            for bisect_index in range(80):
                halfway = 0.5 * (lower + upper)
                halfway_target = radau_target(total, halfway)
                if lower_target * halfway_target <= 0.0:
                    upper = halfway
                else:
                    lower = halfway
                    lower_target = halfway_target
            roots_found.append(0.5 * (lower + upper))
        left_value = right_value
        left_target = right_target
    roots_found.append(1.0)
    points = [(value + 1.0) / 2.0 for value in roots_found]
    quad_rows = []
    for node_index in range(total):
        row_values = []
        for basis_index in range(total):
            coefs = [1.0]
            for other_index in range(total):
                if other_index != basis_index:
                    scale = 1.0 / (points[basis_index] - points[other_index])
                    shifted = [0.0] + coefs
                    widened = coefs + [0.0]
                    coefs = [
                        (shifted[k] - points[other_index] * widened[k]) * scale
                        for k in range(len(shifted))
                    ]
            integral = 0.0
            for power_index in range(len(coefs)):
                integral += (
                    coefs[power_index] * points[node_index] ** (power_index + 1) / (power_index + 1)
                )
            row_values.append(integral)
        quad_rows.append(row_values)
    return (np.array(points), np.array(quad_rows))


LANES = 128
LEAD_LIMIT = 60 * 2**20


def by_node(values):
    values = [float(np.float32(v)) for v in values]
    node = lax.axis_index("node")
    result = jnp.float32(values[0])
    for k, value in enumerate(values[1:], 1):
        result = jnp.where(node == k, jnp.float32(value), result)
    return result


def neighbour_sum(above, tile, below):
    rows, columns = tile.shape
    row = lax.broadcasted_iota(jnp.int32, tile.shape, 0)
    up = jnp.where(row == 0, above, pltpu.roll(tile, 1, 0))
    down = jnp.where(row == rows - 1, below, pltpu.roll(tile, rows - 1, 0))
    return (up + down) + (pltpu.roll(tile, 1, 1) + pltpu.roll(tile, columns - 1, 1))


def tile_slopes(u_rows, v_rows, feed, kill):
    above_u, u, below_u = u_rows
    above_v, v, below_v = v_rows
    product = u * v * v
    slope_u = diffusion[0] * (neighbour_sum(above_u, u, below_u) - 4.0 * u)
    slope_v = diffusion[1] * (neighbour_sum(above_v, v, below_v) - 4.0 * v)
    slope_u = slope_u + (feed * (1.0 - u) - product)
    slope_v = slope_v + (product - (feed + kill) * v)
    return slope_u, slope_v


def rows_of(ref, species, start, before, after):
    length = ref.shape[1]
    above = before[species] if start == 0 else ref[species, start - 1 : start]
    stop = start + TILE
    below = after[species] if stop == length else ref[species, stop : stop + 1]
    return above, ref[species, start:stop], below


def lead_kernel(starts, sections, feed, kill, out_u, out_v, first, last, w, f, k, tail, sems):
    low, high = starts[0], starts[-1] + TILE
    rows = sections.shape[1]
    copies = [
        pltpu.make_async_copy(sections.at[:, 0 : high + TILE], w, sems.at[0]),
        pltpu.make_async_copy(feed.at[low:high], f, sems.at[1]),
        pltpu.make_async_copy(kill.at[low:high], k, sems.at[2]),
        pltpu.make_async_copy(sections.at[:, rows - TILE : rows], tail, sems.at[3]),
    ]
    for copy in copies:
        copy.start()
    for copy in copies:
        copy.wait()
    for n, start in enumerate(starts):
        here = slice(n * TILE, (n + 1) * TILE)
        slope_u, slope_v = tile_slopes(
            rows_of(w, 0, start, None, None), rows_of(w, 1, start, None, None), f[here], k[here]
        )
        out_u[here] = slope_u
        out_v[here] = slope_v
    first[...] = w[:, 0:1]
    last[...] = tail[:, TILE - 1 : TILE]


def lead_slopes(starts, sections, feed_rate, kill_rate):
    columns = sections.shape[-1]
    count = len(starts) * TILE
    shape = lambda *s: jax.ShapeDtypeStruct(s, jnp.float32)
    return pl.pallas_call(
        partial(lead_kernel, starts),
        in_specs=[pl.BlockSpec(memory_space=pltpu.HBM)] * 3,
        out_shape=[shape(count, columns)] * 2 + [shape(2, 1, columns)] * 2,
        scratch_shapes=[
            pltpu.VMEM((2, starts[-1] + 2 * TILE, columns), jnp.float32),
            pltpu.VMEM((count, columns), jnp.float32),
            pltpu.VMEM((count, columns), jnp.float32),
            pltpu.VMEM((2, TILE, columns), jnp.float32),
            pltpu.SemaphoreType.DMA((4,)),
        ],
        compiler_params=pltpu.CompilerParams(vmem_limit_bytes=LEAD_LIMIT),
    )(sections, feed_rate, kill_rate)


def slopes_kernel(groups, before, after, sections, feed, kill, *outs):
    for group, starts in enumerate(groups):
        for k, start in enumerate(starts):
            slope_u, slope_v = tile_slopes(
                rows_of(sections, 0, start, before, after),
                rows_of(sections, 1, start, before, after),
                feed[start : start + TILE],
                kill[start : start + TILE],
            )
            outs[2 * group][k * TILE : (k + 1) * TILE] = slope_u
            outs[2 * group + 1][k * TILE : (k + 1) * TILE] = slope_v


def slopes_of(groups, before, after, sections, feed_rate, kill_rate):
    columns = sections.shape[-1]
    shapes = []
    for starts in groups:
        shapes += [jax.ShapeDtypeStruct((len(starts) * TILE, columns), jnp.float32)] * 2
    return pl.pallas_call(
        partial(slopes_kernel, groups),
        out_shape=shapes,
        compiler_params=pltpu.CompilerParams(vmem_limit_bytes=16 * 2**20),
    )(before, after, sections, feed_rate, kill_rate)


def combined(weights, fields):
    value = weights[0] * fields[0]
    for weight, field in zip(weights[1:], fields[1:]):
        value = value + weight * field
    return value


def tiles(ref):
    return [slice(k, k + TILE) for k in range(0, ref.shape[-2], TILE)]


def message_kernel(tables, counts, *refs):
    refs = list(refs)
    fields = [[refs.pop(0) for _ in range(count)] for count in counts]
    for table, sources in zip(tables, fields):
        for s in range(1, table.shape[1]):
            out = refs.pop(0)
            weights = [by_node(table[:, s, g]) for g in range(len(sources))]
            for here in tiles(out):
                out[here] = combined(weights, [source[here] for source in sources])


def messages(tables, fields):
    counts = tuple(len(f) for f in fields)
    number = sum(table.shape[1] - 1 for table in tables)
    like = fields[0][0]
    return pl.pallas_call(
        partial(message_kernel, tables, counts),
        out_shape=[jax.ShapeDtypeStruct(like.shape, like.dtype)] * number,
        compiler_params=pltpu.CompilerParams(vmem_limit_bytes=12 * 2**20),
    )(*fields[0], *fields[1])


def local_kernel(tables, counts, starts, initial, sections, *refs):
    refs = list(refs)
    fields = [[refs.pop(0) for _ in range(count)] for count in counts]
    (out,) = refs
    for species in range(2):
        sources = fields[species]
        weights = [by_node(tables[species][:, 0, g]) for g in range(len(sources))]
        for start, here in zip(starts, tiles(out)):
            there = slice(start, start + TILE)
            difference = initial[species, there] - sections[species, there]
            out[species, here] = difference + combined(weights, [f[here] for f in sources])


def local_part(tables, starts, initial, sections, fields):
    counts = tuple(len(f) for f in fields)
    like = fields[0][0]
    return pl.pallas_call(
        partial(local_kernel, tables, counts, starts),
        out_shape=jax.ShapeDtypeStruct((2,) + like.shape, like.dtype),
        compiler_params=pltpu.CompilerParams(vmem_limit_bytes=16 * 2**20),
    )(initial, sections, *fields[0], *fields[1])


def residual_kernel(counts, split, maxima, local, *refs):
    refs = list(refs)
    earlier = [refs.pop(0) for _ in range(maxima)]
    sums = [[refs.pop(0) for _ in range(count)] for count in counts]
    largest = refs.pop()
    top = jnp.zeros((TILE, LANES), jnp.float32)
    for ref in earlier:
        top = jnp.maximum(top, ref[...])
    columns = local.shape[-1]
    for species in range(2):
        for n, here in enumerate(tiles(local)):
            for c in range(0, columns, LANES):
                block = (here, slice(c, c + LANES))
                value = local[(species,) + block]
                for part in sums[species]:
                    value = value + part[block]
                if split:
                    refs[n][species, :, c : c + LANES] = value
                else:
                    refs[0][(species,) + block] = value
                top = jnp.maximum(top, jnp.abs(value))
    largest[...] = top


def residual_of(local, sums, split, earlier=()):
    counts = tuple(len(s) for s in sums)
    _, rows, columns = local.shape
    pieces = rows // TILE if split else 1
    shape = lambda *s: jax.ShapeDtypeStruct(s, jnp.float32)
    return pl.pallas_call(
        partial(residual_kernel, counts, split, len(earlier)),
        out_shape=[shape(2, rows // pieces, columns)] * pieces + [shape(TILE, LANES)],
        compiler_params=pltpu.CompilerParams(vmem_limit_bytes=12 * 2**20),
    )(local, *earlier, *sums[0], *sums[1])


def sweep_kernel(species, places, table, stage, *refs):
    if stage == 1:
        before, after, *refs = refs
        pieces, (first, odd, even) = refs[: len(places)], refs[-3:]
    elif stage == 2:
        first, odd, sections = refs[:3]
        out, even, spare, result, sems = refs[-5:]
        late_targets = (even, spare)
    else:
        before, after, sections, *refs = refs
        pieces = refs[: len(places)]
        out, first, even, odd, result, sems = refs[-6:]
    inverse = by_node(1.0 / (4.0 * table[:, species] + 1.0))
    gain = by_node(table[:, species] / (4.0 * table[:, species] + 1.0))
    total, columns = first.shape
    if stage != 2:
        first[0:TILE] = before[species] * inverse
        first[total - TILE : total] = after[species] * inverse
        for piece, starts in zip(pieces, places):
            for k, start in enumerate(starts):
                scaled = piece[species, k * TILE : (k + 1) * TILE] * inverse
                first[start + TILE : start + 2 * TILE] = scaled

    row = lax.broadcasted_iota(jnp.int32, (TILE, LANES), 0)
    lane = lax.broadcasted_iota(jnp.int32, (TILE, LANES), 1)
    blocks = columns // LANES

    def update(source, start, store):
        above_at = pl.ds(pl.multiple_of(jnp.maximum(start - TILE, 0), TILE), TILE)
        below_at = pl.ds(pl.multiple_of(jnp.minimum(start + TILE, total - TILE), TILE), TILE)
        here = pl.ds(start, TILE)
        cut = lambda b: slice((b % blocks) * LANES, (b % blocks + 1) * LANES)
        load = lambda b: source[here, cut(b)]
        right = lambda x: pltpu.roll(x, 1, 1)
        left = lambda x: pltpu.roll(x, LANES - 1, 1)
        tile, following = load(0), load(1)
        tile_left = left(tile)
        before_right = right(load(blocks - 1))
        for b in range(blocks):
            tile_right = right(tile)
            following_left = left(following)
            west = jnp.where(lane == 0, before_right, tile_right)
            east = jnp.where(lane == LANES - 1, following_left, tile_left)
            up = pltpu.roll(jnp.where(row == TILE - 1, source[above_at, cut(b)], tile), 1, 0)
            down = pltpu.roll(jnp.where(row == 0, source[below_at, cut(b)], tile), TILE - 1, 0)
            store(cut(b), first[here, cut(b)] + gain * ((up + down) + (west + east)))
            before_right, tile, tile_left = tile_right, following, following_left
            following = load(b + 2)

    source = odd if stage == 2 else first
    for sweep in {0: range(SWEEPS - 2), 1: range(2), 2: range(2, SWEEPS - 2)}[stage]:
        target = (even, odd)[sweep % 2] if stage != 2 else late_targets[sweep % 2]

        def one_tile(t, _, source=source, target=target):
            start = pl.multiple_of(t * TILE, TILE)

            def store(at, value):
                target[pl.ds(start, TILE), at] = value

            update(source, start, store)
            return 0

        lax.fori_loop(0, total // TILE, one_tile, 0, unroll=5)
        source = target

    if stage == 1:
        return

    def last_tile(t, _):
        start = pl.multiple_of(t * TILE, TILE)

        def store(at, value):
            result[pl.ds(start, TILE), at] = sections[species, pl.ds(start, TILE), at] + value

        update(source, pl.multiple_of(start + TILE, TILE), store)
        return 0

    count = total // TILE - 2
    bounds = (0, count // 2, count)
    copies = []
    for part in range(2):
        lax.fori_loop(bounds[part], bounds[part + 1], last_tile, 0, unroll=4)
        span = slice(bounds[part] * TILE, bounds[part + 1] * TILE)
        copies.append(
            pltpu.make_async_copy(result.at[span], out.at[species, span], sems.at[part])
        )
        copies[-1].start()
    for copy in copies:
        copy.wait()


def swept(species, places, table, before, after, sections, pieces, out):
    _, rows, columns = sections.shape
    total = rows + 2 * TILE
    operands = [before, after, sections, *pieces]
    specs = [pl.BlockSpec(memory_space=pltpu.VMEM)] * len(operands)
    aliases = {}
    if out is not None:
        aliases = {len(operands): 0}
        operands.append(out)
        specs.append(pl.BlockSpec(memory_space=pltpu.HBM))
    return pl.pallas_call(
        partial(sweep_kernel, species, places, table, 0),
        in_specs=specs,
        out_specs=pl.BlockSpec(memory_space=pltpu.HBM),
        out_shape=jax.ShapeDtypeStruct(sections.shape, jnp.float32),
        input_output_aliases=aliases,
        scratch_shapes=[pltpu.VMEM((total, columns), jnp.float32)] * 3
        + [pltpu.VMEM((rows, columns), jnp.float32), pltpu.SemaphoreType.DMA((2,))],
        compiler_params=pltpu.CompilerParams(vmem_limit_bytes=20 * 2**20),
    )(*operands)


def swept_early(species, places, table, before, after, sections, pieces):
    _, rows, columns = sections.shape
    state = (rows + 2 * TILE, columns)
    return pl.pallas_call(
        partial(sweep_kernel, species, places, table, 1),
        out_shape=[jax.ShapeDtypeStruct(state, jnp.float32)] * 2,
        scratch_shapes=[pltpu.VMEM(state, jnp.float32)],
        compiler_params=pltpu.CompilerParams(vmem_limit_bytes=20 * 2**20),
    )(before, after, *pieces)


def swept_late(species, places, table, first, source, sections, out):
    _, rows, columns = sections.shape
    specs = [pl.BlockSpec(memory_space=pltpu.VMEM)] * 3
    return pl.pallas_call(
        partial(sweep_kernel, species, places, table, 2),
        in_specs=specs + [pl.BlockSpec(memory_space=pltpu.HBM)],
        out_specs=pl.BlockSpec(memory_space=pltpu.HBM),
        out_shape=jax.ShapeDtypeStruct(sections.shape, jnp.float32),
        input_output_aliases={3: 0},
        scratch_shapes=[
            pltpu.VMEM(first.shape, jnp.float32),
            pltpu.VMEM(first.shape, jnp.float32),
            pltpu.VMEM((rows, columns), jnp.float32),
            pltpu.SemaphoreType.DMA((2,)),
        ],
        compiler_params=pltpu.CompilerParams(vmem_limit_bytes=20 * 2**20),
    )(first, source, sections, out)


def shifted(array, axis, outer, inner, by_outer, by_inner):
    pairs = []
    for i in range(outer):
        for j in range(inner):
            target = ((i + by_outer) % outer) * inner + (j + by_inner) % inner
            pairs.append((i * inner + j, target))
    return lax.ppermute(array, axis, pairs)


def factored(total):
    inner = next(b for b in range(1, total + 1) if total % b == 0 and b * b >= total)
    return total // inner, inner


def exchange_tables(total, quad):
    outer, inner = factored(total)
    node = np.arange(total)
    high, low = node // inner, node % inner
    index = lambda i, j: (i % outer) * inner + j % inner
    table_u = np.zeros((total, outer, inner))
    table_v = np.zeros((total, inner, outer))
    for s in range(outer):
        for g in range(inner):
            table_u[:, s, g] = quad[index(high + s, low), index(high, low - g)]
            table_v[:, g, s] = quad[index(high, low + g), index(high - s, low)]
    return step_size * table_u, step_size * table_v


def spread_pairs(size, shift):
    if size & (size - 1) == 0:
        return [(i, i ^ shift) for i in range(size)]
    return [(i, (i + shift) % size) for i in range(size)]


def spread_rounds(size):
    covered = 1
    while covered < size:
        shifts = [s * covered for s in (1, 2, 3) if s * covered < size]
        yield shifts
        covered *= len(shifts) + 1


def shards(initial, sections, feed_rate, kill_rate):
    own = sections[0]
    _, rows, columns = own.shape
    nodes = lax.axis_size("node")
    spaces = lax.axis_size("space")
    outer, inner = factored(nodes)
    points, quad = radau_table(nodes)
    coupling = step_size * points[:, None] * np.array(diffusion)[None]
    tables = exchange_tables(nodes, quad)

    edges = (0, rows - TILE)
    middle = list(range(TILE, rows - TILE, TILE))
    half = (2 * len(middle) + 2) // 3
    lead, rest = tuple(middle[:half]), tuple(middle[half:])
    places = (lead, edges, rest)

    along_inner = lambda a, s: shifted(a, "node", outer, inner, 0, s)
    along_outer = lambda a, s: shifted(a, "node", outer, inner, s, 0)

    def gather(u, v):
        fields_u = [u] + [along_inner(u, s) for s in range(1, inner)]
        fields_v = [v] + [along_outer(v, s) for s in range(1, outer)]
        return fields_u, fields_v

    def exchange(fields):
        sent = messages(tables, fields)
        sums_u = [along_outer(sent[s - 1], s) for s in range(1, outer)]
        sums_v = [along_inner(sent[outer - 2 + s], s) for s in range(1, inner)]
        return sums_u, sums_v

    upward = [(i, (i + 1) % spaces) for i in range(spaces)]
    downward = [(j, i) for i, j in upward]
    lead_u, lead_v, first, last = lead_slopes(lead, own, feed_rate, kill_rate)
    gathered = [gather(lead_u, lead_v)]
    late, _ = lax.optimization_barrier((own, lead_u))
    before = lax.ppermute(late[:, rows - 1 :], "space", upward)
    after = lax.ppermute(late[:, :1], "space", downward)
    out = slopes_of((edges, rest), before, after, own, feed_rate, kill_rate)
    gathered += [gather(*out[:2]), gather(*out[2:])]
    sums = [exchange(fields) for fields in gathered]
    local = [
        local_part(tables, starts, initial, own, fields)
        for starts, fields in zip(places, gathered)
    ]

    low, high, edge_largest = residual_of(local[1], sums[1], True)
    low_edge = lax.ppermute(high, "space", upward)
    high_edge = lax.ppermute(low, "space", downward)
    lead_residual, lead_largest = residual_of(local[0], sums[0], False)
    low_edge, high_edge, lead_largest, edge_largest, last_sums = lax.optimization_barrier(
        (low_edge, high_edge, lead_largest, edge_largest, sums[2])
    )
    rest_residual, largest = residual_of(
        local[2], last_sums, False, (lead_largest, edge_largest)
    )

    def spread(value, axis, between=None):
        size = lax.axis_size(axis)
        for shifts in spread_rounds(size):
            others = [
                lax.ppermute(value, axis, spread_pairs(size, s))
                for s in shifts
            ]
            if between:
                between(others)
            for other in others:
                value = jnp.maximum(value, other)
        return value

    pieces = [lead_residual, low, high, rest_residual]
    spots = (lead, edges[:1], edges[1:], rest)
    largest = spread(largest, "node")
    new = swept(0, spots, coupling, low_edge, high_edge, own, pieces, None)
    largest, new = lax.optimization_barrier((largest, new))
    pieces, new = lax.optimization_barrier((pieces, new))
    start, state = swept_early(1, spots, coupling, low_edge, high_edge, own, pieces)
    hold = []

    def between(others):
        nonlocal start, state
        if not hold:
            hold.append(True)
            others[0], start, state = lax.optimization_barrier((others[0], start, state))

    largest = spread(largest, "space", between)
    new = swept_late(1, spots, coupling, start, state, own, new)
    return new[None], jnp.max(largest)


def solution(mesh):
    placed = (
        P(None, "space", None),
        P("node", None, "space", None),
        P("space", None),
        P("space", None),
    )
    return jax.shard_map(
        shards,
        mesh=mesh,
        in_specs=placed,
        out_specs=(P("node", None, "space", None), P()),
        check_vma=False,
    )
```
